32 devices in a mesh: ep: 8 (over z, y), fsdp: 4 (over x, core).
Axes of the slice: x: 2, y: 2, z: 4, core: 2. Of those that a mesh axis runs over, the one named last changes fastest.
Arguments:
- train_gate: float32 [64, 2048, 1024], P('ep', 'fsdp'), may hold values from -0.1875 to 0.1875
- other_gate: float32 [64, 2048, 1024], P('ep', 'fsdp'), may hold values from -0.125 to 0.125
- train_up: float32 [64, 2048, 1024], P('ep', 'fsdp'), may hold values from -0.1875 to 0.1875
- other_up: float32 [64, 2048, 1024], P('ep', 'fsdp'), may hold values from -0.125 to 0.125
- mix_share: float32 [64], P('ep'), may hold values from 0.2 to 0.8
- router_weight: float32 [2048, 64], P('fsdp', 'ep'), may hold values from -0.125 to 0.125
- router_gain: float32 [2048], P('fsdp'), may hold values from 0.25 to 1.75
Outputs:
- ready_gate: bfloat16 [64, 2048, 1024], P('ep')
- ready_up: bfloat16 [64, 2048, 1024], P('ep')
- scale_gate: float32 [64, 1024], P('ep')
- scale_up: float32 [64, 1024], P('ep')
- serve_router: bfloat16 [2048, 64], replicated
The draws below stay inside these ranges and needn't reach their ends.
All inputs are finite; a program needn't handle non-finite values. Where the reference program divides by a largest or mean magnitude, that divisor is 1e-20 or more.
Results may differ from the reference program's by a relative error of at most 0.001.
Values may be sent and summed in bfloat16 or wider, within the bound.
No kernel may reach another device: no remote copies, remote signals or barrier semaphores. Data moves between devices by JAX's collectives and lax.ppermute only.
A program may use at most 256 MiB of HBM per device.

```python
import jax
import jax.numpy as jnp

EXPERTS = 64
D_MODEL = 2048
D_EXPERT = 1024


def with_spikes(drawn, stream_key, source, target, shards_of, factor):
    owner, partner = [(jnp.arange(drawn.shape[dim]) // (drawn.shape[dim] // shards_of)).reshape([-1 if axis == dim else 1 for axis in range(drawn.ndim)]) for dim in (source, target)]
    chosen = jax.random.permutation(stream_key, shards_of)[partner]
    strong = (owner == chosen) | (owner == (partner + shards_of // 2) % shards_of)
    return jnp.where(strong, factor * drawn, drawn)


def steps_of(key, dims, split, least, top_value):
    def one(position, shards_of):
        steps = jax.random.uniform(jax.random.fold_in(jax.random.fold_in(key, 6), position), (shards_of,), jnp.float32, least / len(split), top_value / len(split))
        return jnp.repeat(jnp.exp(steps), dims[position] // shards_of).reshape((-1,) + (1,) * (len(dims) - position - 1))

    gain = one(*split[0])
    for cut in split[1:]:
        gain = gain * one(*cut)
    return gain


def bell_draw(key, shape, spread, bound, pieces=(), dtype=jnp.bfloat16):
    result = jax.random.normal(key, shape, jnp.float32) * spread
    if len(pieces) > 0:
        result = steps_of(key, shape, pieces, -0.22, 0.18) * result
    return jnp.clip(result, min=-bound, max=bound).astype(dtype)


def bell_draw_with(stream_key, dims, width, reach, cuts, heavy, kind=jnp.bfloat16):
    drawn = width * jax.random.normal(stream_key, dims, jnp.float32)
    if cuts:
        drawn = drawn * steps_of(stream_key, dims, cuts, -0.22, 0.18)
    return jnp.clip(with_spikes(drawn, jax.random.fold_in(stream_key, 3), *heavy), -reach, reach).astype(kind)


def setup_inputs(seed: int = 0) -> dict:
    arg_keys = jax.random.split(jax.random.key(seed), 8)
    train_gate = bell_draw_with(arg_keys[0], (EXPERTS, D_MODEL, D_EXPERT), D_MODEL ** -0.5, 0.1875, ((0, 8), (1, 4)), (1, 2, 4, 2.0), jnp.float32)
    other_gate = bell_draw(arg_keys[1], (EXPERTS, D_MODEL, D_EXPERT), D_MODEL ** -0.5, 0.125, ((0, 8), (1, 4)), jnp.float32)
    train_up = bell_draw_with(arg_keys[2], (EXPERTS, D_MODEL, D_EXPERT), D_MODEL ** -0.5, 0.1875, ((0, 8), (1, 4)), (1, 2, 4, 2.0), jnp.float32)
    other_up = bell_draw(arg_keys[3], (EXPERTS, D_MODEL, D_EXPERT), D_MODEL ** -0.5, 0.125, ((0, 8), (1, 4)), jnp.float32)
    mix_share = jnp.clip(0.2 + 0.6 * jax.random.uniform(arg_keys[4], (EXPERTS,), jnp.float32) ** steps_of(arg_keys[4], (EXPERTS,), ((0, 8),), -0.2, 0.2), 0.2, 0.8)
    router_weight = bell_draw(arg_keys[5], (D_MODEL, EXPERTS), D_MODEL ** -0.5, 0.125, ((0, 4), (1, 8)), jnp.float32)
    router_gain = jnp.clip(1.0 + 0.15 * jax.random.normal(arg_keys[6], (D_MODEL,), jnp.float32), 0.25, 1.75)
    return dict(train_gate=train_gate, other_gate=other_gate, train_up=train_up, other_up=other_up, mix_share=mix_share, router_weight=router_weight, router_gain=router_gain)


def reference(train_gate, other_gate, train_up, other_up, mix_share, router_weight, router_gain):
    latest_gate = mix_share[:, None, None] * train_gate + (1.0 - mix_share[:, None, None]) * other_gate
    latest_up = mix_share[:, None, None] * train_up + (1.0 - mix_share[:, None, None]) * other_up
    scale_gate = jnp.max(jnp.abs(latest_gate), axis=1)
    ready_gate = (latest_gate / jnp.expand_dims(scale_gate, 1)).astype(jnp.bfloat16)
    scale_up = jnp.max(jnp.abs(latest_up), axis=1)
    ready_up = (latest_up / jnp.expand_dims(scale_up, 1)).astype(jnp.bfloat16)
    serve_router = (router_weight * router_gain[:, None]).astype(jnp.bfloat16)
    return ready_gate, ready_up, scale_gate, scale_up, serve_router
```

```python
import functools

import jax
import jax.numpy as jnp
from jax import lax
from jax.experimental import pallas as pl
from jax.experimental.pallas import tpu as pltpu
from jax.sharding import PartitionSpec as P


ANY = pl.BlockSpec(memory_space=pl.ANY)
SMEM = pl.BlockSpec(memory_space=pltpu.SMEM)
SUB = 8


def rows_per_step(rows, most):
    return max(d for d in range(16, min(rows, most) + 1, 16) if rows % d == 0)


def mixed(share, train, other):
    return share * train + (1.0 - share) * other


def max_kernel(first, steps, mix_ref, train_ref, other_ref, top_ref, held):
    share = mix_ref[first + pl.program_id(0)]
    r = pl.program_id(1)

    def magnitude(i):
        rows = pl.ds(i * SUB, SUB)
        return jnp.abs(mixed(share, train_ref[0, rows], other_ref[0, rows]))

    top = magnitude(0)
    for i in range(1, train_ref.shape[1] // SUB):
        top = jnp.maximum(top, magnitude(i))
    if steps > 1:
        top = jnp.where(r == 0, top, jnp.maximum(top, held[...]))
        held[...] = top

    @pl.when(r == steps - 1)
    def _():
        top_ref[0] = jnp.max(top, axis=0, keepdims=True)


def local_max(mix_share, train, other, first, count):
    _, rows, cols = train.shape
    step = rows_per_step(rows, 128 if count == 1 else 256)
    block = pl.BlockSpec((1, step, cols), lambda e, r: (first + e, r, 0))
    return pl.pallas_call(
        functools.partial(max_kernel, first, rows // step),
        out_shape=jax.ShapeDtypeStruct((count, 1, cols), jnp.float32),
        grid=(count, rows // step),
        in_specs=[SMEM, block, block],
        out_specs=pl.BlockSpec((1, 1, cols), lambda e, r: (e, 0, 0)),
        scratch_shapes=[pltpu.VMEM((SUB, cols), jnp.float32)],
        cost_estimate=pl.CostEstimate(
            flops=5 * count * rows * cols, bytes_accessed=8 * count * rows * cols, transcendentals=0
        ),
        name="local_max",
    )(mix_share, train, other)


def narrow_kernel(first, tops, place_ref, mix_ref, *refs):
    top_refs, (train_ref, other_ref), (send_ref, whole_ref) = refs[:tops], refs[tops : tops + 2], refs[-2:]
    top = top_refs[0][0]
    for ref in top_refs[1:]:
        top = jnp.maximum(top, ref[0])
    scale = jnp.broadcast_to(1.0 / top, (2 * SUB, top.shape[1]))
    share = mix_ref[first + pl.program_id(0)]
    for i in range(train_ref.shape[1] // (2 * SUB)):
        rows = pl.ds(i * 2 * SUB, 2 * SUB)
        part = (mixed(share, train_ref[0, rows], other_ref[0, rows]) * scale).astype(jnp.bfloat16)
        send_ref[0, rows] = part
        whole_ref[0, rows] = part


def narrow(place, mix_share, tops, at, train, other, piece, parts, whole):
    first, count, low, height = piece
    experts, rows, cols = train.shape
    step = rows_per_step(height, 128 if count == 1 else 256)
    block = pl.BlockSpec((1, step, cols), lambda e, r, place: (first + e, low // step + r, 0))
    held = [] if whole is None else [whole]
    return pl.pallas_call(
        functools.partial(narrow_kernel, first, len(tops)),
        out_shape=(
            jax.ShapeDtypeStruct((count, height, cols), jnp.bfloat16),
            jax.ShapeDtypeStruct((experts, parts * rows, cols), jnp.bfloat16),
        ),
        grid_spec=pltpu.PrefetchScalarGridSpec(
            num_scalar_prefetch=1,
            grid=(count, height // step),
            in_specs=[SMEM]
            + [pl.BlockSpec((1, 1, cols), lambda e, r, place: (at + e, 0, 0))] * len(tops)
            + [block, block]
            + [ANY] * len(held),
            out_specs=(
                pl.BlockSpec((1, step, cols), lambda e, r, place: (e, r, 0)),
                pl.BlockSpec(
                    (1, step, cols),
                    lambda e, r, place: (first + e, place[0] * (rows // step) + low // step + r, 0),
                ),
            ),
        ),
        input_output_aliases={4 + len(tops): 1} if held else {},
        cost_estimate=pl.CostEstimate(
            flops=6 * count * height * cols, bytes_accessed=12 * count * height * cols, transcendentals=0
        ),
        name="narrow",
    )(place, mix_share, *tops, train, other, *held)


def put_kernel(sources, place_ref, *refs):
    for k in range(sources):

        @pl.when(pl.program_id(0) == k)
        def _():
            refs[-1][...] = refs[k][...]


def put(place, arrays, slots, piece, rows, whole):
    first, count, low, height = piece
    cols = whole.shape[2]

    def source(k):
        return pl.BlockSpec(
            (1, height, cols),
            lambda s, e, place: (jnp.where(s < k, 0, jnp.where(s > k, count - 1, e)), 0, 0),
        )

    def target(s, e, place):
        slot = place[slots[0]]
        for k in range(1, len(slots)):
            slot = jnp.where(s == k, place[slots[k]], slot)
        return (first + e, slot * (rows // height) + low // height, 0)

    size = len(arrays) * count * height * cols
    return pl.pallas_call(
        functools.partial(put_kernel, len(arrays)),
        out_shape=jax.ShapeDtypeStruct(whole.shape, whole.dtype),
        grid_spec=pltpu.PrefetchScalarGridSpec(
            num_scalar_prefetch=1,
            grid=(len(arrays), count),
            in_specs=[source(k) for k in range(len(arrays))] + [ANY],
            out_specs=pl.BlockSpec((1, height, cols), target),
        ),
        input_output_aliases={1 + len(arrays): 0},
        cost_estimate=pl.CostEstimate(flops=size, bytes_accessed=4 * size, transcendentals=0),
        name="put",
    )(place, *arrays, whole)


def plan(experts, rows):
    half = rows // 2
    split = [(0, half), (half, rows - half)]

    def runs(lo, hi, most):
        return [(e, min(most, hi - e)) for e in range(lo, hi, most)]

    groups = [(0, 0, 1)]
    groups += [(0, e, n) for e, n in runs(1, min(3, experts), 2)]
    groups += [(0, e, n) for e, n in runs(3, experts, experts)]
    groups += [(1, 0, experts)]
    pieces = [(0, (0, 1, low, height)) for low, height in split]
    pieces += [(0, (e, n, 0, rows)) for e, n in runs(1, min(3, experts), 1)]
    pieces += [(0, (e, n, 0, rows)) for e, n in runs(3, experts, 3)]
    tail = max(experts - 2, 0)
    pieces += [(1, (e, n, 0, rows)) for e, n in runs(0, tail, 3)]
    pieces += [(1, (e, n, 0, rows)) for e, n in runs(tail, experts - 1, 1)]
    pieces += [(1, (experts - 1, 1, low, height)) for low, height in split]
    return groups, pieces


def group_of(groups, array, expert):
    return next(g for g, (a, e, n) in enumerate(groups) if a == array and e <= expert < e + n)


def per_device(parts, train_gate, other_gate, train_up, other_up, mix_share, router_weight, router_gain):
    experts, rows, _ = train_gate.shape
    inner = 2 if parts % 2 == 0 else 1
    outer = parts // inner
    me = lax.axis_index("fsdp")
    power = parts & (parts - 1) == 0
    groups, pieces = plan(experts, rows)

    def step(k, l):
        return [(i, (i // inner + k) % outer * inner + (i % inner ^ l)) for i in range(parts)]

    def send(x, k, l):
        return lax.ppermute(x, "fsdp", step(k, l))

    def partner(s):
        return [(i, i ^ s if power else (i + s) % parts) for i in range(parts)]

    steps = [[dict((b, a) for a, b in step(k, l)) for l in range(inner)] for k in range(outer)]
    table = [[steps[k][l][i] for k in range(outer) for l in range(inner)] for i in range(parts)]
    place = jnp.asarray(table, jnp.int32)[me]

    train, other = (train_gate, train_up), (other_gate, other_up)
    tops = []
    for g, (a, first, count) in enumerate(groups):
        top = [local_max(mix_share, train[a], other[a], first, count)]
        for s in range(1, parts):
            top.append(lax.ppermute(top[0], "fsdp", partner(s)))
        tops.append(top)

    whole = [None, None]
    sent = []
    for a, piece in pieces:
        g = group_of(groups, a, piece[0])
        own, whole[a] = narrow(
            place, mix_share, tops[g], piece[0] - groups[g][1], train[a], other[a], piece, parts, whole[a]
        )
        sent.append(own)

    for i, (a, piece) in enumerate(pieces):
        arrays, slots = [], []
        if inner == 2:
            arrays.append(send(sent[i], 0, 1))
            slots.append(1)
        for k in range(1, outer):
            far = send(sent[i], k, 0)
            arrays.append(far)
            slots.append(inner * k)
            if inner == 2:
                arrays.append(send(far, 0, 1))
                slots.append(inner * k + 1)
        if not arrays:
            continue
        cut = len(arrays) - 1 if inner == 2 and i + 1 == len(pieces) else 0
        if cut:
            whole[a] = put(place, arrays[:cut], slots[:cut], piece, rows, whole[a])
        whole[a] = put(place, arrays[cut:], slots[cut:], piece, rows, whole[a])

    scales = [
        jnp.concatenate(
            [functools.reduce(jnp.maximum, top)[:, 0] for top, (b, _, _) in zip(tops, groups) if b == a], axis=0
        )
        for a in range(2)
    ]
    part_router = (router_weight * router_gain[:, None]).astype(jnp.bfloat16)
    wide = lax.all_gather(part_router, "ep", axis=1, tiled=True)
    serve_router = jnp.zeros((parts * rows, wide.shape[1]), wide.dtype)
    serve_router = lax.dynamic_update_slice(serve_router, wide, (me * rows, 0))
    for s in range(1, parts):
        piece = lax.ppermute(wide, "fsdp", partner(s))
        source = jnp.asarray([dict((b, a) for a, b in partner(s))[i] for i in range(parts)], jnp.int32)[me]
        serve_router = lax.dynamic_update_slice(serve_router, piece, (source * rows, 0))
    return whole[0], whole[1], scales[0], scales[1], serve_router


def solution(mesh):
    parts = mesh.shape["fsdp"]
    placed = (
        P("ep", "fsdp", None),
        P("ep", "fsdp", None),
        P("ep", "fsdp", None),
        P("ep", "fsdp", None),
        P("ep"),
        P("fsdp", "ep"),
        P("fsdp"),
    )
    return jax.shard_map(
        functools.partial(per_device, parts),
        mesh=mesh,
        in_specs=placed,
        out_specs=(P("ep", None, None), P("ep", None, None), P("ep", None), P("ep", None), P()),
        check_vma=False,
    )
```

```python
import functools

import jax
import jax.numpy as jnp
from jax import lax
from jax.experimental import pallas as pl
from jax.experimental.pallas import tpu as pltpu
from jax.sharding import PartitionSpec as P


ANY = pl.BlockSpec(memory_space=pl.ANY)
HBM = pl.BlockSpec(memory_space=pltpu.HBM)
SMEM = pl.BlockSpec(memory_space=pltpu.SMEM)
SUB = 8
PARAMS = pltpu.CompilerParams(vmem_limit_bytes=48 * 2**20)


def mixed(share, train, other):
    return share * train + (1.0 - share) * other


def fetches(first, low, height, blocks, sources, held, sems):
    step = height // blocks
    return [
        [
            pltpu.make_async_copy(
                ref.at[first, pl.ds(low + j * step, step)], held.at[k, pl.ds(j * step, step)], sems.at[k, j]
            )
            for k, ref in enumerate(sources)
        ]
        for j in range(blocks)
    ]


def first_max_kernel(first, blocks, mix_ref, train_ref, other_ref, top_ref, share_ref, held, sems, mix_sem):
    rows = held.shape[1]
    step = rows // blocks
    copies = fetches(first, 0, rows, blocks, (train_ref, other_ref), held, sems)
    for pair in copies:
        for copy in pair:
            copy.start()
    mix = pltpu.make_async_copy(mix_ref, share_ref, mix_sem)
    mix.start()
    mix.wait()
    share = share_ref[first]
    top = jnp.zeros((SUB, held.shape[2]), jnp.float32)
    for j, pair in enumerate(copies):
        for copy in pair:
            copy.wait()

        def body(i, top):
            at = pl.ds(pl.multiple_of(j * step + i * SUB, SUB), SUB)
            return jnp.maximum(top, jnp.abs(mixed(share, held[0, at], held[1, at])))

        top = lax.fori_loop(0, step // SUB, body, top, unroll=4)
    top_ref[...] = jnp.max(top, axis=0, keepdims=True)


def first_max(mix_share, train, other, first):
    _, rows, cols = train.shape
    blocks = 4
    return pl.pallas_call(
        functools.partial(first_max_kernel, first, blocks),
        out_shape=jax.ShapeDtypeStruct((1, cols), jnp.float32),
        in_specs=[HBM, HBM, HBM],
        scratch_shapes=[
            pltpu.SMEM(mix_share.shape, jnp.float32),
            pltpu.VMEM((2, rows, cols), jnp.float32),
            pltpu.SemaphoreType.DMA((2, blocks)),
            pltpu.SemaphoreType.DMA,
        ],
        compiler_params=PARAMS,
        cost_estimate=pl.CostEstimate(flops=5 * rows * cols, bytes_accessed=8 * rows * cols, transcendentals=0),
        name="first_max",
    )(mix_share, train, other)


def max_kernel(first, mix_ref, train_ref, other_ref, top_ref):
    e = pl.program_id(0)
    share = mix_ref[first + e]

    def body(i, top):
        at = pl.ds(pl.multiple_of(i * SUB, SUB), SUB)
        return jnp.maximum(top, jnp.abs(mixed(share, train_ref[0, at], other_ref[0, at])))

    rows, cols = train_ref.shape[1:]
    top = lax.fori_loop(0, rows // SUB, body, jnp.zeros((SUB, cols), jnp.float32), unroll=4)
    top_ref[pl.ds(e, 1)] = jnp.max(top, axis=0, keepdims=True)


def local_max(mix_share, train, other, first, count):
    _, rows, cols = train.shape
    block = pl.BlockSpec((1, rows, cols), lambda e: (first + e, 0, 0))
    return pl.pallas_call(
        functools.partial(max_kernel, first),
        out_shape=jax.ShapeDtypeStruct((count, cols), jnp.float32),
        grid=(count,),
        in_specs=[SMEM, block, block],
        out_specs=pl.BlockSpec((count, cols), lambda e: (0, 0)),
        compiler_params=PARAMS,
        cost_estimate=pl.CostEstimate(
            flops=5 * count * rows * cols, bytes_accessed=8 * count * rows * cols, transcendentals=0
        ),
        name="local_max",
    )(mix_share, train, other)


def top_of(refs, at):
    top = refs[0][pl.ds(at, 1)]
    for ref in refs[1:]:
        top = jnp.maximum(top, ref[pl.ds(at, 1)])
    return top


def first_narrow_kernel(tops, piece, blocks, mix_ref, *refs):
    first, _, low, height = piece
    top_refs, (train_ref, other_ref, send_ref, share_ref, held, sems, mix_sem) = refs[:tops], refs[tops:]
    step = height // blocks
    copies = fetches(first, low, height, blocks, (train_ref, other_ref), held, sems)
    b = pl.program_id(0)
    mix = pltpu.make_async_copy(mix_ref, share_ref, mix_sem)

    @pl.when(b == 0)
    def _():
        for pair in copies:
            for copy in pair:
                copy.start()
        mix.start()
        mix.wait()

    for j, pair in enumerate(copies):

        @pl.when(b == j)
        def _():
            for copy in pair:
                copy.wait()

    share = share_ref[first]
    scale = jnp.broadcast_to(1.0 / top_of(top_refs, 0), (2 * SUB, held.shape[2]))

    def body(i, carry):
        at = pl.ds(pl.multiple_of(b * step + i * 2 * SUB, 2 * SUB), 2 * SUB)
        part = mixed(share, held[0, at], held[1, at]) * scale
        send_ref[0, pl.ds(pl.multiple_of(i * 2 * SUB, 2 * SUB), 2 * SUB)] = part.astype(jnp.bfloat16)
        return carry

    lax.fori_loop(0, step // (2 * SUB), body, 0, unroll=2)


def first_narrow(mix_share, tops, train, other, piece):
    cols = train.shape[2]
    height = piece[3]
    blocks = 2
    return pl.pallas_call(
        functools.partial(first_narrow_kernel, len(tops), piece, blocks),
        out_shape=jax.ShapeDtypeStruct((1, height, cols), jnp.bfloat16),
        grid=(blocks,),
        in_specs=[HBM] + [pl.BlockSpec((1, cols), lambda b: (0, 0))] * len(tops) + [HBM, HBM],
        out_specs=pl.BlockSpec((1, height // blocks, cols), lambda b: (0, b, 0)),
        scratch_shapes=[
            pltpu.SMEM(mix_share.shape, jnp.float32),
            pltpu.VMEM((2, height, cols), jnp.float32),
            pltpu.SemaphoreType.DMA((2, blocks)),
            pltpu.SemaphoreType.DMA,
        ],
        compiler_params=PARAMS,
        cost_estimate=pl.CostEstimate(flops=6 * height * cols, bytes_accessed=10 * height * cols, transcendentals=0),
        name="first_narrow",
    )(mix_share, *tops, train, other)


def narrow_kernel(first, at, tops, place_ref, mix_ref, *refs):
    top_refs, (train_ref, other_ref), (send_ref, whole_ref) = refs[:tops], refs[tops : tops + 2], refs[-2:]
    e = pl.program_id(0)
    height, cols = train_ref.shape[1:]
    scale = jnp.broadcast_to(1.0 / top_of(top_refs, at + e), (2 * SUB, cols))
    share = mix_ref[first + e]

    def body(i, carry):
        rows = pl.ds(pl.multiple_of(i * 2 * SUB, 2 * SUB), 2 * SUB)
        part = (mixed(share, train_ref[0, rows], other_ref[0, rows]) * scale).astype(jnp.bfloat16)
        send_ref[0, rows] = part
        whole_ref[0, rows] = part
        return carry

    lax.fori_loop(0, height // (2 * SUB), body, 0, unroll=2)


def narrow(place, mix_share, tops, at, train, other, piece, parts, whole):
    first, count, low, height = piece
    experts, rows, cols = train.shape
    step = max(d for d in (height, height // 2) if d <= 256 or d == height // 2)
    step = step if low % step == 0 and rows % step == 0 else rows // 4
    block = pl.BlockSpec((1, step, cols), lambda e, r, place: (first + e, low // step + r, 0))
    held = [] if whole is None else [whole]
    return pl.pallas_call(
        functools.partial(narrow_kernel, first, at, len(tops)),
        out_shape=(
            jax.ShapeDtypeStruct((count, height, cols), jnp.bfloat16),
            jax.ShapeDtypeStruct((experts, parts * rows, cols), jnp.bfloat16),
        ),
        grid_spec=pltpu.PrefetchScalarGridSpec(
            num_scalar_prefetch=1,
            grid=(count, height // step),
            in_specs=[SMEM]
            + [pl.BlockSpec(top.shape, lambda e, r, place: (0, 0)) for top in tops]
            + [block, block]
            + [ANY] * len(held),
            out_specs=(
                pl.BlockSpec((1, step, cols), lambda e, r, place: (e, r, 0)),
                pl.BlockSpec(
                    (1, step, cols),
                    lambda e, r, place: (first + e, place[0] * (rows // step) + low // step + r, 0),
                ),
            ),
        ),
        input_output_aliases={4 + len(tops): 1} if held else {},
        compiler_params=PARAMS,
        cost_estimate=pl.CostEstimate(
            flops=6 * count * height * cols, bytes_accessed=12 * count * height * cols, transcendentals=0
        ),
        name="narrow",
    )(place, mix_share, *tops, train, other, *held)


def put_kernel(slots, piece, rows, place_ref, *refs):
    first, count, low, height = piece
    whole_ref, held, in_sems, out_sems = refs[-4:]
    items = [(s, e) for s in range(len(slots)) for e in range(count)]
    reads, writes = [], []
    for i, (s, e) in enumerate(items):
        reads.append(pltpu.make_async_copy(refs[s].at[e], held.at[i], in_sems.at[i]))
        start = pl.multiple_of(place_ref[slots[s]] * rows + low, 2 * SUB)
        target = whole_ref.at[first + e, pl.ds(start, height)]
        writes.append(pltpu.make_async_copy(held.at[i], target, out_sems.at[i]))
    for read in reads:
        read.start()
    for read, write in zip(reads, writes):
        read.wait()
        write.start()
    for write in writes:
        write.wait()


def put(place, arrays, slots, piece, rows, whole):
    _, count, _, height = piece
    cols = whole.shape[2]
    n = len(arrays) * count
    return pl.pallas_call(
        functools.partial(put_kernel, tuple(slots), piece, rows),
        out_shape=jax.ShapeDtypeStruct(whole.shape, whole.dtype),
        in_specs=[SMEM] + [ANY] * (len(arrays) + 1),
        out_specs=ANY,
        scratch_shapes=[
            pltpu.VMEM((n, height, cols), jnp.bfloat16),
            pltpu.SemaphoreType.DMA((n,)),
            pltpu.SemaphoreType.DMA((n,)),
        ],
        input_output_aliases={1 + len(arrays): 0},
        compiler_params=PARAMS,
        cost_estimate=pl.CostEstimate(flops=n * height * cols, bytes_accessed=4 * n * height * cols, transcendentals=0),
        name="put",
    )(place, *arrays, whole)


def scales_kernel(groups, parts, *refs):
    for g, (a, first, count) in enumerate(groups):
        tops = refs[g * parts : (g + 1) * parts]
        top = tops[0][...]
        for ref in tops[1:]:
            top = jnp.maximum(top, ref[...])
        refs[len(groups) * parts + a][pl.ds(first, count)] = top


def all_scales(tops, groups, experts, cols):
    flat = [top for group in tops for top in group]
    shape = jax.ShapeDtypeStruct((experts, cols), jnp.float32)
    return pl.pallas_call(
        functools.partial(scales_kernel, groups, len(tops[0])),
        out_shape=(shape, shape),
        compiler_params=PARAMS,
        cost_estimate=pl.CostEstimate(flops=8 * experts * cols, bytes_accessed=64 * experts * cols, transcendentals=0),
        name="scales",
    )(*flat)


def keep_kernel(x_ref, y_ref):
    y_ref[...] = x_ref[...]


def keep(x):
    return pl.pallas_call(
        keep_kernel,
        out_shape=jax.ShapeDtypeStruct(x.shape, x.dtype),
        compiler_params=PARAMS,
        cost_estimate=pl.CostEstimate(flops=x.size, bytes_accessed=4 * x.size, transcendentals=0),
        name="keep",
    )(x)


def plan(experts, rows):
    def runs(lo, hi, most):
        return [(e, min(most, hi - e)) for e in range(lo, hi, most)]

    def split(cut):
        return [(0, cut), (cut, rows - cut)]

    groups = [(0, 0, 1)]
    groups += [(0, e, n) for e, n in runs(1, min(3, experts), 2)]
    groups += [(0, e, n) for e, n in runs(3, experts, experts)]
    groups += [(1, 0, experts)]
    pieces = [(0, (0, 1, low, height)) for low, height in split(rows // 2)]
    pieces += [(0, (e, n, 0, rows)) for e, n in runs(1, min(3, experts), 1)]
    pieces += [(0, (e, n, 0, rows)) for e, n in runs(3, experts, 3)]
    tail = max(experts - 2, 0)
    pieces += [(1, (e, n, 0, rows)) for e, n in runs(0, tail, 3)]
    pieces += [(1, (e, n, 0, rows)) for e, n in runs(tail, experts - 1, 1)]
    pieces += [(1, (experts - 1, 1, low, height)) for low, height in split(rows - rows // 4)]
    return groups, pieces


def group_of(groups, array, expert):
    return next(g for g, (a, e, n) in enumerate(groups) if a == array and e <= expert < e + n)


def per_device(parts, train_gate, other_gate, train_up, other_up, mix_share, router_weight, router_gain):
    experts, rows, cols = train_gate.shape
    inner = 2 if parts % 2 == 0 else 1
    outer = parts // inner
    me = lax.axis_index("fsdp")
    groups, pieces = plan(experts, rows)

    def step(k, l):
        return [(i, (i // inner + k) % outer * inner + (i % inner ^ l)) for i in range(parts)]

    def spread(x):
        got = [x]
        if inner == 2:
            got.append(lax.ppermute(x, "fsdp", step(0, 1)))
        for k in range(1, outer):
            got.append(lax.ppermute(x, "fsdp", step(k, 0)))
            if inner == 2:
                got.append(lax.ppermute(got[-1], "fsdp", step(0, 1)))
        return got

    steps = [[dict((b, a) for a, b in step(k, l)) for l in range(inner)] for k in range(outer)]
    table = [[steps[k][l][i] for k in range(outer) for l in range(inner)] for i in range(parts)]
    place = jnp.asarray(table, jnp.int32)[me]

    train, other = (train_gate, train_up), (other_gate, other_up)
    tops = []
    for g, (a, first, count) in enumerate(groups):
        if g == 0:
            top = first_max(mix_share, train[a], other[a], first)
        else:
            top = local_max(mix_share, train[a], other[a], first, count)
        if g > 0:
            tops.append(spread(top))
            continue
        direct = [top]
        for s in range(1, parts):
            direct.append(lax.ppermute(top, "fsdp", step(s // inner, s % inner)))
        tops.append(direct)

    whole = [None, None]
    got = []
    for i, (a, piece) in enumerate(pieces):
        g = group_of(groups, a, piece[0])
        if i == 0:
            own = first_narrow(mix_share, tops[g], train[a], other[a], piece)
        else:
            own, whole[a] = narrow(
                place, mix_share, tops[g], piece[0] - groups[g][1], train[a], other[a], piece, parts, whole[a]
            )
        got.append(spread(own))

    for i, (a, piece) in enumerate(pieces):
        slots = list(range(0 if i == 0 else 1, parts))
        cut = len(slots) - 1 if i + 1 == len(pieces) else 0
        for some in (slots[:cut], slots[cut:]):
            if some:
                whole[a] = put(place, [got[i][j] for j in some], some, piece, rows, whole[a])

    scales = all_scales(tops, groups, experts, cols)
    part_router = (router_weight * router_gain[:, None]).astype(jnp.bfloat16)
    row_router = jnp.zeros((parts * rows, part_router.shape[1]), jnp.bfloat16)
    for j, x in enumerate(spread(part_router)):
        row_router = lax.dynamic_update_slice(row_router, x, (place[j] * rows, 0))
    wide_router = lax.all_gather(row_router, "ep", axis=1, tiled=True)
    serve_router = keep(wide_router.T).T
    return whole[0], whole[1], scales[0], scales[1], serve_router


def solution(mesh):
    parts = mesh.shape["fsdp"]
    placed = (
        P("ep", "fsdp", None),
        P("ep", "fsdp", None),
        P("ep", "fsdp", None),
        P("ep", "fsdp", None),
        P("ep"),
        P("fsdp", "ep"),
        P("fsdp"),
    )
    return jax.shard_map(
        functools.partial(per_device, parts),
        mesh=mesh,
        in_specs=placed,
        out_specs=(P("ep", None, None), P("ep", None, None), P("ep", None), P("ep", None), P()),
        check_vma=False,
    )
```

```python
import functools
import math

import jax
import jax.numpy as jnp
from jax import lax
from jax.experimental import pallas as pl
from jax.experimental.pallas import tpu as pltpu
from jax.sharding import PartitionSpec as P


ANY = pl.BlockSpec(memory_space=pl.ANY)
HBM = pl.BlockSpec(memory_space=pltpu.HBM)
SMEM = pl.BlockSpec(memory_space=pltpu.SMEM)
SUB = 8
PARAMS = pltpu.CompilerParams(vmem_limit_bytes=48 * 2**20)


def mixed(share, train, other):
    return share * train + (1.0 - share) * other


def fetches(first, low, height, blocks, sources, held, sems):
    step = height // blocks
    return [
        [
            pltpu.make_async_copy(
                ref.at[first, pl.ds(low + j * step, step)], held.at[k, pl.ds(j * step, step)], sems.at[k, j]
            )
            for k, ref in enumerate(sources)
        ]
        for j in range(blocks)
    ]


def first_max_kernel(first, blocks, mix_ref, train_ref, other_ref, top_ref, early_ref, share_ref, held, early, sems, mix_sem, early_sem):
    rows = held.shape[1]
    step = rows // blocks
    copies = fetches(first, 0, rows, blocks, (train_ref, other_ref), held, sems)
    for pair in copies:
        for copy in pair:
            copy.start()
    mix = pltpu.make_async_copy(mix_ref, share_ref, mix_sem)
    mix.start()
    mix.wait()
    share = share_ref[first]
    top = jnp.zeros((SUB, held.shape[2]), jnp.float32)
    leave = pltpu.make_async_copy(early, early_ref, early_sem)
    for j, pair in enumerate(copies):
        for copy in pair:
            copy.wait()

        def body(i, top):
            at = pl.ds(pl.multiple_of(j * step + i * SUB, SUB), SUB)
            return jnp.maximum(top, jnp.abs(mixed(share, held[0, at], held[1, at])))

        def mix_rows(i, carry):
            at = pl.ds(pl.multiple_of(i * SUB, SUB), SUB)
            early[at] = mixed(share, held[0, at], held[1, at])
            return carry

        if j == 0:
            lax.fori_loop(0, early.shape[0] // SUB, mix_rows, 0, unroll=2)
        top = lax.fori_loop(0, step // SUB, body, top, unroll=4)
        if j == 1:
            leave.start()
    top_ref[...] = jnp.max(top, axis=0, keepdims=True)
    leave.wait()


def first_max(mix_share, train, other, first, early):
    _, rows, cols = train.shape
    blocks = 4
    return pl.pallas_call(
        functools.partial(first_max_kernel, first, blocks),
        out_shape=(
            jax.ShapeDtypeStruct((1, cols), jnp.float32),
            jax.ShapeDtypeStruct((early, cols), jnp.float32),
        ),
        in_specs=[HBM, HBM, HBM],
        out_specs=(pl.BlockSpec(memory_space=pltpu.VMEM), ANY),
        scratch_shapes=[
            pltpu.SMEM(mix_share.shape, jnp.float32),
            pltpu.VMEM((2, rows, cols), jnp.float32),
            pltpu.VMEM((early, cols), jnp.float32),
            pltpu.SemaphoreType.DMA((2, blocks)),
            pltpu.SemaphoreType.DMA,
            pltpu.SemaphoreType.DMA,
        ],
        compiler_params=PARAMS,
        cost_estimate=pl.CostEstimate(flops=5 * rows * cols, bytes_accessed=8 * rows * cols, transcendentals=0),
        name="first_max",
    )(mix_share, train, other)


def max_kernel(first, mix_ref, train_ref, other_ref, top_ref):
    e = pl.program_id(0)
    share = mix_ref[first + e]

    def body(i, top):
        at = pl.ds(pl.multiple_of(i * SUB, SUB), SUB)
        return jnp.maximum(top, jnp.abs(mixed(share, train_ref[0, at], other_ref[0, at])))

    rows, cols = train_ref.shape[1:]
    top = lax.fori_loop(0, rows // SUB, body, jnp.zeros((SUB, cols), jnp.float32), unroll=4)
    top_ref[pl.ds(e, 1)] = jnp.max(top, axis=0, keepdims=True)


def local_max(mix_share, train, other, first, count):
    _, rows, cols = train.shape
    block = pl.BlockSpec((1, rows, cols), lambda e: (first + e, 0, 0))
    return pl.pallas_call(
        functools.partial(max_kernel, first),
        out_shape=jax.ShapeDtypeStruct((count, cols), jnp.float32),
        grid=(count,),
        in_specs=[SMEM, block, block],
        out_specs=pl.BlockSpec((count, cols), lambda e: (0, 0)),
        compiler_params=PARAMS,
        cost_estimate=pl.CostEstimate(
            flops=5 * count * rows * cols, bytes_accessed=8 * count * rows * cols, transcendentals=0
        ),
        name="local_max",
    )(mix_share, train, other)


def top_of(refs, at):
    top = refs[0][pl.ds(at, 1)]
    for ref in refs[1:]:
        top = jnp.maximum(top, ref[pl.ds(at, 1)])
    return top


def first_narrow_kernel(tops, piece, blocks, mix_ref, *refs):
    first, _, low, height = piece
    top_refs, (train_ref, other_ref, send_ref, share_ref, held, sems, mix_sem) = refs[:tops], refs[tops:]
    step = height // blocks
    copies = fetches(first, low, height, blocks, (train_ref, other_ref), held, sems)
    b = pl.program_id(0)
    mix = pltpu.make_async_copy(mix_ref, share_ref, mix_sem)

    @pl.when(b == 0)
    def _():
        for pair in copies:
            for copy in pair:
                copy.start()
        mix.start()
        mix.wait()

    for j, pair in enumerate(copies):

        @pl.when(b == j)
        def _():
            for copy in pair:
                copy.wait()

    share = share_ref[first]
    scale = jnp.broadcast_to(1.0 / top_of(top_refs, 0), (2 * SUB, held.shape[2]))

    def body(i, carry):
        at = pl.ds(pl.multiple_of(b * step + i * 2 * SUB, 2 * SUB), 2 * SUB)
        part = mixed(share, held[0, at], held[1, at]) * scale
        send_ref[0, pl.ds(pl.multiple_of(i * 2 * SUB, 2 * SUB), 2 * SUB)] = part.astype(jnp.bfloat16)
        return carry

    lax.fori_loop(0, step // (2 * SUB), body, 0, unroll=2)


def first_narrow(mix_share, tops, train, other, piece):
    cols = train.shape[2]
    height = piece[3]
    blocks = 2
    return pl.pallas_call(
        functools.partial(first_narrow_kernel, len(tops), piece, blocks),
        out_shape=jax.ShapeDtypeStruct((1, height, cols), jnp.bfloat16),
        grid=(blocks,),
        in_specs=[HBM] + [pl.BlockSpec((1, cols), lambda b: (0, 0))] * len(tops) + [HBM, HBM],
        out_specs=pl.BlockSpec((1, height // blocks, cols), lambda b: (0, b, 0)),
        scratch_shapes=[
            pltpu.SMEM(mix_share.shape, jnp.float32),
            pltpu.VMEM((2, height, cols), jnp.float32),
            pltpu.SemaphoreType.DMA((2, blocks)),
            pltpu.SemaphoreType.DMA,
        ],
        compiler_params=PARAMS,
        cost_estimate=pl.CostEstimate(flops=6 * height * cols, bytes_accessed=10 * height * cols, transcendentals=0),
        name="first_narrow",
    )(mix_share, *tops, train, other)


def narrow_kernel(first, at, tops, place_ref, mix_ref, *refs):
    top_refs, (train_ref, other_ref), (send_ref, whole_ref) = refs[:tops], refs[tops : tops + 2], refs[-2:]
    e = pl.program_id(0)
    height, cols = train_ref.shape[1:]
    scale = jnp.broadcast_to(1.0 / top_of(top_refs, at + e), (2 * SUB, cols))
    share = mix_ref[first + e]

    def body(i, carry):
        rows = pl.ds(pl.multiple_of(i * 2 * SUB, 2 * SUB), 2 * SUB)
        part = (mixed(share, train_ref[0, rows], other_ref[0, rows]) * scale).astype(jnp.bfloat16)
        send_ref[0, rows] = part
        whole_ref[0, rows] = part
        return carry

    lax.fori_loop(0, height // (2 * SUB), body, 0, unroll=2)


def narrow(place, mix_share, tops, at, train, other, piece, parts, whole):
    first, count, low, height = piece
    experts, rows, cols = train.shape
    common = math.gcd(height, low, rows)
    step = max(d for d in range(16, min(common, 256) + 1, 16) if common % d == 0)
    block = pl.BlockSpec((1, step, cols), lambda e, r, place: (first + e, low // step + r, 0))
    held = [] if whole is None else [whole]
    return pl.pallas_call(
        functools.partial(narrow_kernel, first, at, len(tops)),
        out_shape=(
            jax.ShapeDtypeStruct((count, height, cols), jnp.bfloat16),
            jax.ShapeDtypeStruct((experts, parts * rows, cols), jnp.bfloat16),
        ),
        grid_spec=pltpu.PrefetchScalarGridSpec(
            num_scalar_prefetch=1,
            grid=(count, height // step),
            in_specs=[SMEM]
            + [pl.BlockSpec(top.shape, lambda e, r, place: (0, 0)) for top in tops]
            + [block, block]
            + [ANY] * len(held),
            out_specs=(
                pl.BlockSpec((1, step, cols), lambda e, r, place: (e, r, 0)),
                pl.BlockSpec(
                    (1, step, cols),
                    lambda e, r, place: (first + e, place[0] * (rows // step) + low // step + r, 0),
                ),
            ),
        ),
        input_output_aliases={4 + len(tops): 1} if held else {},
        compiler_params=PARAMS,
        cost_estimate=pl.CostEstimate(
            flops=6 * count * height * cols, bytes_accessed=12 * count * height * cols, transcendentals=0
        ),
        name="narrow",
    )(place, mix_share, *tops, train, other, *held)


def finish_kernel(parts, place_ref, *refs):
    tops, rows, whole_ref = refs[:parts], refs[parts : 2 * parts], refs[-1]
    scale = jnp.broadcast_to(1.0 / top_of(tops, 0), (2 * SUB, whole_ref.shape[2]))
    for j in range(parts):

        @pl.when(pl.program_id(0) == j)
        def _():
            def body(i, carry):
                at = pl.ds(pl.multiple_of(i * 2 * SUB, 2 * SUB), 2 * SUB)
                whole_ref[0, at] = (rows[j][at] * scale).astype(jnp.bfloat16)
                return carry

            lax.fori_loop(0, whole_ref.shape[1] // (2 * SUB), body, 0)


def finish(place, tops, mixed_rows, expert, rows, whole):
    early, cols = mixed_rows[0].shape
    parts = len(mixed_rows)
    return pl.pallas_call(
        functools.partial(finish_kernel, parts),
        out_shape=jax.ShapeDtypeStruct(whole.shape, whole.dtype),
        grid_spec=pltpu.PrefetchScalarGridSpec(
            num_scalar_prefetch=1,
            grid=(parts,),
            in_specs=[pl.BlockSpec((1, cols), lambda j, place: (0, 0))] * parts
            + [pl.BlockSpec((early, cols), lambda j, place: (0, 0))] * parts
            + [ANY],
            out_specs=pl.BlockSpec((1, early, cols), lambda j, place: (expert, place[j] * (rows // early), 0)),
        ),
        input_output_aliases={1 + 2 * parts: 0},
        compiler_params=PARAMS,
        cost_estimate=pl.CostEstimate(
            flops=2 * parts * early * cols, bytes_accessed=6 * parts * early * cols, transcendentals=0
        ),
        name="finish",
    )(place, *tops, *mixed_rows, whole)


def put_kernel(slots, piece, rows, place_ref, *refs):
    first, count, low, height = piece
    whole_ref, held, in_sems, out_sems = refs[-4:]
    items = [(s, e) for s in range(len(slots)) for e in range(count)]
    reads, writes = [], []
    for i, (s, e) in enumerate(items):
        reads.append(pltpu.make_async_copy(refs[s].at[e], held.at[i], in_sems.at[i]))
        start = pl.multiple_of(place_ref[slots[s]] * rows + low, 2 * SUB)
        target = whole_ref.at[first + e, pl.ds(start, height)]
        writes.append(pltpu.make_async_copy(held.at[i], target, out_sems.at[i]))
    for read in reads:
        read.start()
    for read, write in zip(reads, writes):
        read.wait()
        write.start()
    for write in writes:
        write.wait()


def put(place, arrays, slots, piece, rows, whole):
    _, count, _, height = piece
    cols = whole.shape[2]
    n = len(arrays) * count
    return pl.pallas_call(
        functools.partial(put_kernel, tuple(slots), piece, rows),
        out_shape=jax.ShapeDtypeStruct(whole.shape, whole.dtype),
        in_specs=[SMEM] + [ANY] * (len(arrays) + 1),
        out_specs=ANY,
        scratch_shapes=[
            pltpu.VMEM((n, height, cols), jnp.bfloat16),
            pltpu.SemaphoreType.DMA((n,)),
            pltpu.SemaphoreType.DMA((n,)),
        ],
        input_output_aliases={1 + len(arrays): 0},
        compiler_params=PARAMS,
        cost_estimate=pl.CostEstimate(flops=n * height * cols, bytes_accessed=4 * n * height * cols, transcendentals=0),
        name="put",
    )(place, *arrays, whole)


def scales_kernel(groups, parts, *refs):
    for g, (a, first, count) in enumerate(groups):
        tops = refs[g * parts : (g + 1) * parts]
        top = tops[0][...]
        for ref in tops[1:]:
            top = jnp.maximum(top, ref[...])
        refs[len(groups) * parts + a][pl.ds(first, count)] = top


def all_scales(tops, groups, experts, cols):
    flat = [top for group in tops for top in group]
    shape = jax.ShapeDtypeStruct((experts, cols), jnp.float32)
    return pl.pallas_call(
        functools.partial(scales_kernel, groups, len(tops[0])),
        out_shape=(shape, shape),
        compiler_params=PARAMS,
        cost_estimate=pl.CostEstimate(flops=8 * experts * cols, bytes_accessed=64 * experts * cols, transcendentals=0),
        name="scales",
    )(*flat)


def keep_kernel(x_ref, y_ref):
    y_ref[...] = x_ref[...]


def keep(x):
    return pl.pallas_call(
        keep_kernel,
        out_shape=jax.ShapeDtypeStruct(x.shape, x.dtype),
        compiler_params=PARAMS,
        cost_estimate=pl.CostEstimate(flops=x.size, bytes_accessed=4 * x.size, transcendentals=0),
        name="keep",
    )(x)


def plan(experts, rows):
    def runs(lo, hi, most):
        return [(e, min(most, hi - e)) for e in range(lo, hi, most)]

    groups = [(0, 0, 1)]
    groups += [(0, e, n) for e, n in runs(1, min(3, experts), 2)]
    groups += [(0, e, n) for e, n in runs(3, experts, experts)]
    groups += [(1, 0, experts)]
    early = rows // 8
    cut = rows // 2 + early
    pieces = [(0, (0, 1, early, cut - early)), (0, (0, 1, cut, rows - cut))]
    pieces += [(0, (e, n, 0, rows)) for e, n in runs(1, min(3, experts), 1)]
    pieces += [(0, (e, n, 0, rows)) for e, n in runs(3, experts, 3)]
    tail = max(experts - 2, 0)
    pieces += [(1, (e, n, 0, rows)) for e, n in runs(0, tail, 3)]
    pieces += [(1, (e, n, 0, rows)) for e, n in runs(tail, experts - 1, 1)]
    cut = rows - rows // 4
    pieces += [(1, (experts - 1, 1, 0, cut)), (1, (experts - 1, 1, cut, rows - cut))]
    return groups, pieces, early


def group_of(groups, array, expert):
    return next(g for g, (a, e, n) in enumerate(groups) if a == array and e <= expert < e + n)


def last_puts(count, parts):
    return range(count - 2, count) if parts % 2 == 0 and parts > 2 else ()


def per_device(parts, train_gate, other_gate, train_up, other_up, mix_share, router_weight, router_gain):
    experts, rows, cols = train_gate.shape
    inner = 2 if parts % 2 == 0 else 1
    outer = parts // inner
    me = lax.axis_index("fsdp")
    groups, pieces, early = plan(experts, rows)

    def step(k, l):
        return [(i, (i // inner + k) % outer * inner + (i % inner ^ l)) for i in range(parts)]

    def spread(x):
        got = [x]
        if inner == 2:
            got.append(lax.ppermute(x, "fsdp", step(0, 1)))
        for k in range(1, outer):
            got.append(lax.ppermute(x, "fsdp", step(k, 0)))
            if inner == 2:
                got.append(lax.ppermute(got[-1], "fsdp", step(0, 1)))
        return got

    steps = [[dict((b, a) for a, b in step(k, l)) for l in range(inner)] for k in range(outer)]
    table = [[steps[k][l][i] for k in range(outer) for l in range(inner)] for i in range(parts)]
    place = jnp.asarray(table, jnp.int32)[me]

    train, other = (train_gate, train_up), (other_gate, other_up)
    tops = []
    for g, (a, first, count) in enumerate(groups):
        if g == 0:
            top, ahead = first_max(mix_share, train[a], other[a], first, early)
        else:
            top = local_max(mix_share, train[a], other[a], first, count)
        tops.append(spread(top))

    whole = [None, None]
    got = []
    for i, (a, piece) in enumerate(pieces):
        g = group_of(groups, a, piece[0])
        if i == 0:
            own = first_narrow(mix_share, tops[g], train[a], other[a], piece)
        else:
            own, whole[a] = narrow(
                place, mix_share, tops[g], piece[0] - groups[g][1], train[a], other[a], piece, parts, whole[a]
            )
        got.append(spread(own))

    whole[0] = finish(place, tops[0], spread(ahead), groups[0][1], rows, whole[0])

    def place_rows(i, slots):
        a, piece = pieces[i]
        whole[a] = put(place, [got[i][j] for j in slots], slots, piece, rows, whole[a])

    early_puts = last_puts(len(pieces), parts)
    for i in early_puts:
        place_rows(i, [1])
    for i in range(len(pieces)):
        slots = list(range(0 if i == 0 else 2 if i in early_puts else 1, parts))
        if i + 1 == len(pieces) and len(slots) > 1:
            a, (expert, _, low, _) = pieces[i]
            for j in slots:
                whole[a] = lax.dynamic_update_slice(
                    whole[a], got[i][j], (expert, place[j] * rows + low, 0)
                )
        elif slots:
            place_rows(i, slots)

    scales = all_scales(tops, groups, experts, cols)
    part_router = (router_weight * router_gain[:, None]).astype(jnp.bfloat16)
    row_router = jnp.zeros((parts * rows, part_router.shape[1]), jnp.bfloat16)
    for j, x in enumerate(spread(part_router)):
        row_router = lax.dynamic_update_slice(row_router, x, (place[j] * rows, 0))
    wide_router = lax.all_gather(row_router, "ep", axis=1, tiled=True)
    serve_router = keep(wide_router.T).T
    return whole[0], whole[1], scales[0], scales[1], serve_router


def solution(mesh):
    parts = mesh.shape["fsdp"]
    placed = (
        P("ep", "fsdp", None),
        P("ep", "fsdp", None),
        P("ep", "fsdp", None),
        P("ep", "fsdp", None),
        P("ep"),
        P("fsdp", "ep"),
        P("fsdp"),
    )
    return jax.shard_map(
        functools.partial(per_device, parts),
        mesh=mesh,
        in_specs=placed,
        out_specs=(P("ep", None, None), P("ep", None, None), P("ep", None), P("ep", None), P()),
        check_vma=False,
    )
```

```python
import functools
import math

import jax
import jax.numpy as jnp
from jax import lax
from jax.experimental import pallas as pl
from jax.experimental.pallas import tpu as pltpu
from jax.sharding import PartitionSpec as P


ANY = pl.BlockSpec(memory_space=pl.ANY)
HBM = pl.BlockSpec(memory_space=pltpu.HBM)
SMEM = pl.BlockSpec(memory_space=pltpu.SMEM)
SUB = 8
PARAMS = pltpu.CompilerParams(vmem_limit_bytes=48 * 2**20)


def mixed(share, train, other):
    return share * train + (1.0 - share) * other


def first_max_kernel(
    first, mix_ref, train_ref, other_ref, top_ref, kept_ref, early_ref, share_ref, held, early, sems, mix_sem, early_sem
):
    rows, step = held.shape[1], early.shape[0]
    blocks, kept = rows // step, kept_ref.shape[0] // step
    copies = [
        [
            pltpu.make_async_copy(
                ref.at[first, pl.ds(j * step, step)], held.at[k, pl.ds(j * step, step)], sems.at[k, j]
            )
            for k, ref in enumerate((train_ref, other_ref))
        ]
        for j in range(blocks)
    ]
    for pair in copies:
        for copy in pair:
            copy.start()
    mix = pltpu.make_async_copy(mix_ref, share_ref, mix_sem)
    mix.start()
    mix.wait()
    share = share_ref[first]
    top = jnp.zeros((SUB, held.shape[2]), jnp.float32)
    leave = pltpu.make_async_copy(early, early_ref, early_sem)
    for j, pair in enumerate(copies):
        for copy in pair:
            copy.wait()

        def body(i, top):
            at = pl.ds(pl.multiple_of(j * step + i * SUB, SUB), SUB)
            row = mixed(share, held[0, at], held[1, at])
            if j == 0:
                early[pl.ds(pl.multiple_of(i * SUB, SUB), SUB)] = row
            elif j <= kept:
                kept_ref[pl.ds(pl.multiple_of((j - 1) * step + i * SUB, SUB), SUB)] = row
            return jnp.maximum(top, jnp.abs(row))

        top = lax.fori_loop(0, step // SUB, body, top, unroll=4)
        if j == min(2, blocks - 1):
            leave.start()
    top_ref[...] = jnp.max(top, axis=0, keepdims=True)
    leave.wait()


def first_max(mix_share, train, other, first, early, kept):
    _, rows, cols = train.shape
    return pl.pallas_call(
        functools.partial(first_max_kernel, first),
        out_shape=(
            jax.ShapeDtypeStruct((1, cols), jnp.float32),
            jax.ShapeDtypeStruct((kept, cols), jnp.float32),
            jax.ShapeDtypeStruct((early, cols), jnp.float32),
        ),
        in_specs=[HBM, HBM, HBM],
        out_specs=(pl.BlockSpec(memory_space=pltpu.VMEM), pl.BlockSpec(memory_space=pltpu.VMEM), ANY),
        scratch_shapes=[
            pltpu.SMEM(mix_share.shape, jnp.float32),
            pltpu.VMEM((2, rows, cols), jnp.float32),
            pltpu.VMEM((early, cols), jnp.float32),
            pltpu.SemaphoreType.DMA((2, rows // early)),
            pltpu.SemaphoreType.DMA,
            pltpu.SemaphoreType.DMA,
        ],
        compiler_params=PARAMS,
        cost_estimate=pl.CostEstimate(flops=5 * rows * cols, bytes_accessed=8 * rows * cols, transcendentals=0),
        name="first_max",
    )(mix_share, train, other)


def max_kernel(first, mix_ref, train_ref, other_ref, top_ref):
    e = pl.program_id(0)
    share = mix_ref[first + e]

    def body(i, top):
        at = pl.ds(pl.multiple_of(i * SUB, SUB), SUB)
        return jnp.maximum(top, jnp.abs(mixed(share, train_ref[0, at], other_ref[0, at])))

    rows, cols = train_ref.shape[1:]
    top = lax.fori_loop(0, rows // SUB, body, jnp.zeros((SUB, cols), jnp.float32), unroll=4)
    top_ref[pl.ds(e, 1)] = jnp.max(top, axis=0, keepdims=True)


def local_max(mix_share, train, other, first, count):
    _, rows, cols = train.shape
    block = pl.BlockSpec((1, rows, cols), lambda e: (first + e, 0, 0))
    return pl.pallas_call(
        functools.partial(max_kernel, first),
        out_shape=jax.ShapeDtypeStruct((count, cols), jnp.float32),
        grid=(count,),
        in_specs=[SMEM, block, block],
        out_specs=pl.BlockSpec((count, cols), lambda e: (0, 0)),
        compiler_params=PARAMS,
        cost_estimate=pl.CostEstimate(
            flops=5 * count * rows * cols, bytes_accessed=8 * count * rows * cols, transcendentals=0
        ),
        name="local_max",
    )(mix_share, train, other)


def top_of(refs, at):
    top = refs[0][pl.ds(at, 1)]
    for ref in refs[1:]:
        top = jnp.maximum(top, ref[pl.ds(at, 1)])
    return top


def first_narrow_kernel(kept_ref, *refs):
    tops, send_ref = refs[:-1], refs[-1]
    scale = jnp.broadcast_to(1.0 / top_of(tops, 0), (2 * SUB, kept_ref.shape[1]))

    def body(i, carry):
        at = pl.ds(pl.multiple_of(i * 2 * SUB, 2 * SUB), 2 * SUB)
        send_ref[0, at] = (kept_ref[at] * scale).astype(jnp.bfloat16)
        return carry

    lax.fori_loop(0, kept_ref.shape[0] // (2 * SUB), body, 0, unroll=2)


def first_narrow(kept, tops):
    height, cols = kept.shape
    return pl.pallas_call(
        first_narrow_kernel,
        out_shape=jax.ShapeDtypeStruct((1, height, cols), jnp.bfloat16),
        compiler_params=PARAMS,
        cost_estimate=pl.CostEstimate(flops=2 * height * cols, bytes_accessed=6 * height * cols, transcendentals=0),
        name="first_narrow",
    )(kept, *tops)


def narrow_kernel(first, at, tops, place_ref, mix_ref, *refs):
    top_refs, (train_ref, other_ref), (send_ref, whole_ref) = refs[:tops], refs[tops : tops + 2], refs[-2:]
    e = pl.program_id(0)
    height, cols = train_ref.shape[1:]
    scale = jnp.broadcast_to(1.0 / top_of(top_refs, at + e), (2 * SUB, cols))
    share = mix_ref[first + e]

    def body(i, carry):
        rows = pl.ds(pl.multiple_of(i * 2 * SUB, 2 * SUB), 2 * SUB)
        part = (mixed(share, train_ref[0, rows], other_ref[0, rows]) * scale).astype(jnp.bfloat16)
        send_ref[0, rows] = part
        whole_ref[0, rows] = part
        return carry

    lax.fori_loop(0, height // (2 * SUB), body, 0, unroll=2)


def narrow(place, mix_share, tops, at, train, other, piece, parts, whole):
    first, count, low, height = piece
    experts, rows, cols = train.shape
    common = math.gcd(height, low, rows)
    step = max(d for d in range(16, min(common, 256) + 1, 16) if common % d == 0)
    block = pl.BlockSpec((1, step, cols), lambda e, r, place: (first + e, low // step + r, 0))
    held = [] if whole is None else [whole]
    return pl.pallas_call(
        functools.partial(narrow_kernel, first, at, len(tops)),
        out_shape=(
            jax.ShapeDtypeStruct((count, height, cols), jnp.bfloat16),
            jax.ShapeDtypeStruct((experts, parts * rows, cols), jnp.bfloat16),
        ),
        grid_spec=pltpu.PrefetchScalarGridSpec(
            num_scalar_prefetch=1,
            grid=(count, height // step),
            in_specs=[SMEM]
            + [pl.BlockSpec(top.shape, lambda e, r, place: (0, 0)) for top in tops]
            + [block, block]
            + [ANY] * len(held),
            out_specs=(
                pl.BlockSpec((1, step, cols), lambda e, r, place: (e, r, 0)),
                pl.BlockSpec(
                    (1, step, cols),
                    lambda e, r, place: (first + e, place[0] * (rows // step) + low // step + r, 0),
                ),
            ),
        ),
        input_output_aliases={4 + len(tops): 1} if held else {},
        compiler_params=PARAMS,
        cost_estimate=pl.CostEstimate(
            flops=6 * count * height * cols, bytes_accessed=12 * count * height * cols, transcendentals=0
        ),
        name="narrow",
    )(place, mix_share, *tops, train, other, *held)


def finish_kernel(parts, place_ref, *refs):
    tops, rows, whole_ref = refs[:parts], refs[parts : 2 * parts], refs[-1]
    scale = jnp.broadcast_to(1.0 / top_of(tops, 0), (2 * SUB, whole_ref.shape[2]))
    for j in range(parts):

        @pl.when(pl.program_id(0) == j)
        def _():
            def body(i, carry):
                at = pl.ds(pl.multiple_of(i * 2 * SUB, 2 * SUB), 2 * SUB)
                whole_ref[0, at] = (rows[j][at] * scale).astype(jnp.bfloat16)
                return carry

            lax.fori_loop(0, whole_ref.shape[1] // (2 * SUB), body, 0)


def finish(place, tops, mixed_rows, expert, rows, whole):
    early, cols = mixed_rows[0].shape
    parts = len(mixed_rows)
    return pl.pallas_call(
        functools.partial(finish_kernel, parts),
        out_shape=jax.ShapeDtypeStruct(whole.shape, whole.dtype),
        grid_spec=pltpu.PrefetchScalarGridSpec(
            num_scalar_prefetch=1,
            grid=(parts,),
            in_specs=[pl.BlockSpec((1, cols), lambda j, place: (0, 0))] * parts
            + [pl.BlockSpec((early, cols), lambda j, place: (0, 0))] * parts
            + [ANY],
            out_specs=pl.BlockSpec((1, early, cols), lambda j, place: (expert, place[j] * (rows // early), 0)),
        ),
        input_output_aliases={1 + 2 * parts: 0},
        compiler_params=PARAMS,
        cost_estimate=pl.CostEstimate(
            flops=2 * parts * early * cols, bytes_accessed=6 * parts * early * cols, transcendentals=0
        ),
        name="finish",
    )(place, *tops, *mixed_rows, whole)


def put_kernel(slots, piece, rows, place_ref, *refs):
    first, count, low, height = piece
    whole_ref, held, in_sems, out_sems = refs[-4:]
    items = [(s, e) for s in range(len(slots)) for e in range(count)]
    reads, writes = [], []
    for i, (s, e) in enumerate(items):
        reads.append(pltpu.make_async_copy(refs[s].at[e], held.at[i], in_sems.at[i]))
        start = pl.multiple_of(place_ref[slots[s]] * rows + low, 2 * SUB)
        target = whole_ref.at[first + e, pl.ds(start, height)]
        writes.append(pltpu.make_async_copy(held.at[i], target, out_sems.at[i]))
    for read in reads:
        read.start()
    for read, write in zip(reads, writes):
        read.wait()
        write.start()
    for write in writes:
        write.wait()


def put(place, arrays, slots, piece, rows, whole):
    _, count, _, height = piece
    cols = whole.shape[2]
    n = len(arrays) * count
    return pl.pallas_call(
        functools.partial(put_kernel, tuple(slots), piece, rows),
        out_shape=jax.ShapeDtypeStruct(whole.shape, whole.dtype),
        in_specs=[SMEM] + [ANY] * (len(arrays) + 1),
        out_specs=ANY,
        scratch_shapes=[
            pltpu.VMEM((n, height, cols), jnp.bfloat16),
            pltpu.SemaphoreType.DMA((n,)),
            pltpu.SemaphoreType.DMA((n,)),
        ],
        input_output_aliases={1 + len(arrays): 0},
        compiler_params=PARAMS,
        cost_estimate=pl.CostEstimate(flops=n * height * cols, bytes_accessed=4 * n * height * cols, transcendentals=0),
        name="put",
    )(place, *arrays, whole)


def scales_kernel(groups, parts, *refs):
    for g, (a, first, count) in enumerate(groups):
        tops = refs[g * parts : (g + 1) * parts]
        top = tops[0][...]
        for ref in tops[1:]:
            top = jnp.maximum(top, ref[...])
        refs[len(groups) * parts + a][pl.ds(first, count)] = top


def all_scales(tops, groups, experts, cols):
    flat = [top for group in tops for top in group]
    shape = jax.ShapeDtypeStruct((experts, cols), jnp.float32)
    return pl.pallas_call(
        functools.partial(scales_kernel, groups, len(tops[0])),
        out_shape=(shape, shape),
        compiler_params=PARAMS,
        cost_estimate=pl.CostEstimate(flops=8 * experts * cols, bytes_accessed=64 * experts * cols, transcendentals=0),
        name="scales",
    )(*flat)


def keep_kernel(x_ref, y_ref):
    y_ref[...] = x_ref[...]


def keep(x):
    return pl.pallas_call(
        keep_kernel,
        out_shape=jax.ShapeDtypeStruct(x.shape, x.dtype),
        compiler_params=PARAMS,
        cost_estimate=pl.CostEstimate(flops=x.size, bytes_accessed=4 * x.size, transcendentals=0),
        name="keep",
    )(x)


def plan(experts, rows):
    def runs(lo, hi, most):
        return [(e, min(most, hi - e)) for e in range(lo, hi, most)]

    groups = [(0, 0, 1)]
    groups += [(0, e, n) for e, n in runs(1, min(3, experts), 2)]
    groups += [(0, e, n) for e, n in runs(3, experts, experts)]
    groups += [(1, 0, experts)]
    early = rows // 8
    cut = rows // 2 + early
    pieces = [(0, (0, 1, early, cut - early)), (0, (0, 1, cut, rows - cut))]
    pieces += [(0, (e, n, 0, rows)) for e, n in runs(1, min(3, experts), 1)]
    pieces += [(0, (e, n, 0, rows)) for e, n in runs(3, experts, 3)]
    tail = max(experts - 2, 0)
    pieces += [(1, (e, n, 0, rows)) for e, n in runs(0, tail, 3)]
    pieces += [(1, (e, n, 0, rows)) for e, n in runs(tail, experts - 1, 1)]
    cut = rows - rows * 3 // 16 // 16 * 16
    pieces += [(1, (experts - 1, 1, 0, cut)), (1, (experts - 1, 1, cut, rows - cut))]
    return groups, pieces, early


def group_of(groups, array, expert):
    return next(g for g, (a, e, n) in enumerate(groups) if a == array and e <= expert < e + n)


def last_puts(count, parts):
    return range(count - 2, count) if parts % 2 == 0 and parts > 2 else ()


def per_device(parts, train_gate, other_gate, train_up, other_up, mix_share, router_weight, router_gain):
    experts, rows, cols = train_gate.shape
    inner = 2 if parts % 2 == 0 else 1
    outer = parts // inner
    me = lax.axis_index("fsdp")
    groups, pieces, early = plan(experts, rows)

    def step(k, l):
        return [(i, (i // inner + k) % outer * inner + (i % inner ^ l)) for i in range(parts)]

    def spread(x):
        got = [x]
        if inner == 2:
            got.append(lax.ppermute(x, "fsdp", step(0, 1)))
        for k in range(1, outer):
            got.append(lax.ppermute(x, "fsdp", step(k, 0)))
            if inner == 2:
                got.append(lax.ppermute(got[-1], "fsdp", step(0, 1)))
        return got

    steps = [[dict((b, a) for a, b in step(k, l)) for l in range(inner)] for k in range(outer)]
    table = [[steps[k][l][i] for k in range(outer) for l in range(inner)] for i in range(parts)]
    place = jnp.asarray(table, jnp.int32)[me]

    train, other = (train_gate, train_up), (other_gate, other_up)
    tops = []
    for g, (a, first, count) in enumerate(groups):
        if g == 0:
            share = pltpu.with_memory_space_constraint(mix_share, pltpu.HBM) if experts > 1 else mix_share
            top, kept, ahead = first_max(share, train[a], other[a], first, early, pieces[0][1][3])
        else:
            top = local_max(mix_share, train[a], other[a], first, count)
        tops.append(spread(top))

    whole = [None, None]
    got = []
    for i, (a, piece) in enumerate(pieces):
        g = group_of(groups, a, piece[0])
        if i == 0:
            own = first_narrow(kept, tops[g])
        else:
            own, whole[a] = narrow(
                place, mix_share, tops[g], piece[0] - groups[g][1], train[a], other[a], piece, parts, whole[a]
            )
        got.append(spread(own))

    whole[0] = finish(place, tops[0], spread(ahead), groups[0][1], rows, whole[0])

    def place_rows(i, slots):
        a, piece = pieces[i]
        whole[a] = put(place, [got[i][j] for j in slots], slots, piece, rows, whole[a])

    early_puts = last_puts(len(pieces), parts)
    for i in early_puts:
        place_rows(i, [1])
    for i in range(len(pieces)):
        slots = list(range(0 if i == 0 else 2 if i in early_puts else 1, parts))
        if i in early_puts:
            a, (expert, _, low, _) = pieces[i]
            for j in slots:
                whole[a] = lax.dynamic_update_slice(
                    whole[a], got[i][j], (expert, place[j] * rows + low, 0)
                )
        elif slots:
            place_rows(i, slots)

    scales = all_scales(tops, groups, experts, cols)
    part_router = (router_weight * router_gain[:, None]).astype(jnp.bfloat16)
    row_router = jnp.zeros((parts * rows, part_router.shape[1]), jnp.bfloat16)
    for j, x in enumerate(spread(part_router)):
        row_router = lax.dynamic_update_slice(row_router, x, (place[j] * rows, 0))
    wide_router = lax.all_gather(row_router, "ep", axis=1, tiled=True)
    serve_router = keep(wide_router.T).T
    return whole[0], whole[1], scales[0], scales[1], serve_router


def solution(mesh):
    parts = mesh.shape["fsdp"]
    placed = (
        P("ep", "fsdp", None),
        P("ep", "fsdp", None),
        P("ep", "fsdp", None),
        P("ep", "fsdp", None),
        P("ep"),
        P("fsdp", "ep"),
        P("fsdp"),
    )
    return jax.shard_map(
        functools.partial(per_device, parts),
        mesh=mesh,
        in_specs=placed,
        out_specs=(P("ep", None, None), P("ep", None, None), P("ep", None), P("ep", None), P()),
        check_vma=False,
    )
```
